128 devices in a mesh: rows: 16 (over x, y_lo, core), dim: 8 (over y_hi, z).
Axes of the slice: x: 4, y: 4 (y_hi: 2, y_lo: 2; y = y_hi * 2 + y_lo), z: 4, core: 2. Of those that a mesh axis runs over, the one named last changes fastest.
Arguments:
- entity_table: float32 [524288, 512], P(('rows', 'dim')), may hold values from -2.5 to 2.5
- relations: float32 [822, 512], replicated, may hold values from -6 to 6
- thresholds: float32 [64], replicated, may hold values from 0.2 to 2
- head_ids: int32 [2048], replicated, may hold values from 0 to 524287
- rel_ids: int32 [2048], replicated, may hold values from 0 to 821
- thr_idx: int32 [2048], replicated, may hold values from 0 to 63
Outputs:
- serving_table: float32 [524288, 512], P('rows', 'dim')
- fraction: float32 [2048], P(('rows', 'dim'))
The draws below stay inside these ranges and needn't reach their ends.
All inputs are finite; a program needn't handle non-finite values.
Results may differ from the reference program's by a relative error of at most 0.0011.
Values sent between devices are 32-bit elements; how exact they have to be, the bound alone decides.
No kernel may reach another device: no remote copies, remote signals or barrier semaphores. Data moves between devices by JAX's collectives and lax.ppermute only.
A program may use at most 128 MiB of HBM per device.

```python
import math
import jax
import jax.numpy as jnp
from jax import lax

D = 512
ENT_DEV = 4096
Q = 2048
NREL = 822
NTHR = 64
ENT = 524288


cluster_count = 32


def draw_entity_table(key, part):
    key_ids = jax.random.fold_in(key, 11)
    key_cent = jax.random.fold_in(key, 12)
    key_vals = jax.random.fold_in(key, 13)
    key_jit = jax.random.fold_in(key, 14)
    member = jax.random.randint(key_ids, (ENT,), 0, cluster_count)
    centers = jnp.clip(jax.random.normal(key_cent, (cluster_count, D), jnp.float32), -6.0, 6.0)
    shared = jnp.take(centers, member, axis=0)
    position = jnp.arange(ENT, dtype=jnp.float32)[:, None] / ENT
    jitter = jax.random.uniform(key_jit, (ENT, 1), jnp.float32, -0.5, 0.5)
    scale = float(D) ** (-0.25) * jnp.exp(math.log(3.0) * (position - 0.5) + jitter)
    noise = jnp.clip(jax.random.normal(key_vals, (ENT, D), jnp.float32), -6.0, 6.0)
    values = scale * (0.8 * shared + 0.6 * noise)
    return jnp.clip(values, -2.5, 2.5).astype(jnp.float32)


def place_ends(drawn, rng, least, top_value):
    spot = [jax.random.randint(jax.random.fold_in(rng, axis), (), 0, length) for axis, length in enumerate(drawn.shape)]
    widest = drawn.shape.index(max(drawn.shape))
    beside = spot[:widest] + [(spot[widest] + 1) % drawn.shape[widest]] + spot[widest + 1:]
    return drawn.at[tuple(spot)].set(least).at[tuple(beside)].set(top_value)


def scatter_about(stream_key, extent, deviation, reach, held_as=jnp.bfloat16):
    result = deviation * jax.random.normal(stream_key, extent, jnp.float32)
    return jnp.clip(result, min=-reach, max=reach).astype(held_as)


def setup_inputs(seed: int = 0) -> dict:
    key_of = jax.random.split(jax.random.key(seed), 7)
    return {
        "entity_table": draw_entity_table(jax.random.fold_in(key_of[6], 71), 0),
        "relations": scatter_about(key_of[1], (NREL, D), 1.0, 6.0, jnp.float32),
        "thresholds": jnp.clip(jax.random.uniform(key_of[2], (NTHR,), jnp.float32, 0.2, 2.0), 0.2, 2.0),
        "head_ids": place_ends(jax.random.randint(key_of[3], (Q,), 0, ENT), jax.random.fold_in(key_of[3], 1), 0, ENT - 1).astype(jnp.int32),
        "rel_ids": place_ends(jax.random.randint(key_of[4], (Q,), 0, NREL), jax.random.fold_in(key_of[4], 1), 0, NREL - 1).astype(jnp.int32),
        "thr_idx": place_ends(jax.random.randint(key_of[5], (Q,), 0, NTHR), jax.random.fold_in(key_of[5], 1), 0, NTHR - 1).astype(jnp.int32),
    }


sharpness = 2.0


def reference(entity_table, relations, thresholds, head_ids, rel_ids, thr_idx):
    head_vecs = jnp.take(entity_table, head_ids, axis=0)
    query = (head_vecs * jnp.take(relations, rel_ids, axis=0)).astype(jnp.bfloat16)
    query = lax.optimization_barrier(query).astype(jnp.float32)
    level = jnp.take(thresholds, thr_idx)
    block = ENT_DEV * 4
    count = ENT // block
    blocks = entity_table.reshape(count, block, D)

    def step(total, rows_block):
        ent_low = lax.optimization_barrier(rows_block.astype(jnp.bfloat16)).astype(jnp.float32)
        score = jnp.dot(query, ent_low.T, precision=lax.Precision.HIGHEST, preferred_element_type=jnp.float32)
        soft = jax.nn.sigmoid(sharpness * (score - level[:, None]))
        return total + jnp.sum(soft, axis=1), None

    total, unused = lax.scan(step, jnp.zeros((Q,), jnp.float32), blocks)
    return entity_table, total * (1.0 / ENT)
```

```python
import functools

import jax
import jax.numpy as jnp
from jax import lax
from jax.experimental import pallas as pl
from jax.experimental.pallas import tpu as pltpu
from jax.sharding import Mesh
from jax.sharding import PartitionSpec as P


sharpness = 2.0
ALL = ("x", "yl", "c", "yh", "z")
DIM = ("yh", "z")
YZ = ("yl", "yh", "z")
PARTS = ((0, 2048), (2048, 2048))
BLK = 512


def exchange(value, axis):
    return lax.all_to_all(value, axis, split_axis=0, concat_axis=0, tiled=True)


def spread(value, axis):
    count = lax.axis_size(axis)
    copies = jnp.broadcast_to(value[None], (count,) + value.shape)
    return exchange(copies, axis)


HOPS = tuple((dy, dz) for dz in (0, 1, 3, 2) for dy in (0, 1))


def flip_kernel(to_ref, x_ref, *refs):
    outs, turned = refs[:-1], refs[-1]
    turned[...] = x_ref[...].T
    cols = outs[0].shape[0]
    for k, o_ref in enumerate(outs):
        first = pl.multiple_of(to_ref[k] * cols, cols)
        o_ref[...] = turned[pl.ds(first, cols), :]


def flipped(table, to, start, length):
    width = table.shape[1]
    cols = width // len(HOPS)
    first = start // BLK
    spec = pl.BlockSpec((cols, BLK), lambda i, to: (0, i))
    return pl.pallas_call(
        flip_kernel,
        grid_spec=pltpu.PrefetchScalarGridSpec(
            num_scalar_prefetch=1,
            grid=(length // BLK,),
            in_specs=[pl.BlockSpec((BLK, width), lambda i, to: (first + i, 0))],
            out_specs=[spec] * len(HOPS),
            scratch_shapes=[pltpu.VMEM((width, BLK), table.dtype)],
        ),
        out_shape=[jax.ShapeDtypeStruct((cols, length), table.dtype)] * len(HOPS),
        cost_estimate=pl.CostEstimate(flops=0, transcendentals=0, bytes_accessed=8 * width * length),
        name="flip",
    )(to, table)


def place_kernel(start, rows, from_ref, *refs):
    count = len(HOPS)
    parts, out, sems = refs[:count], refs[-2], refs[-1]
    copies = []
    for k, part in enumerate(parts):
        at = pl.multiple_of(from_ref[k] * rows + start, 128)
        copies.append(
            pltpu.make_async_copy(part, out.at[:, pl.ds(at, part.shape[1])], sems.at[k])
        )
    for copy in copies:
        copy.start()
    for copy in copies:
        copy.wait()


def placed(parts, origin, start, rows, held):
    count = len(parts)
    cols = parts[0].shape[0]
    args = list(parts)
    if held is not None:
        args.append(held)
    return pl.pallas_call(
        functools.partial(place_kernel, start, rows),
        in_specs=[pl.BlockSpec(memory_space=pltpu.SMEM)] + [pl.BlockSpec(memory_space=pl.ANY)] * len(args),
        out_specs=pl.BlockSpec(memory_space=pl.ANY),
        out_shape=jax.ShapeDtypeStruct((cols, count * rows), parts[0].dtype),
        scratch_shapes=[pltpu.SemaphoreType.DMA((count,))],
        input_output_aliases={} if held is None else {count + 1: 0},
        name="place",
    )(origin, *args)


def sent(parts):
    got = [parts[0]]
    for (dy, dz), part in list(zip(HOPS, parts))[1:]:
        way = [(y * 4 + z, (y ^ dy) * 4 + (z + dz) % 4) for y in range(2) for z in range(4)]
        got.append(lax.ppermute(part, DIM, way))
    return got


def score_kernel(q_ref, lvl_ref, e_ref, o_ref, ql_ref):
    queries = q_ref.shape[0]

    @pl.when(pl.program_id(0) == 0)
    def _():
        ql_ref[...] = q_ref[...].astype(jnp.bfloat16)
        o_ref[...] = jnp.zeros_like(o_ref)

    ent = e_ref[...].astype(jnp.bfloat16)
    score = lax.dot_general(
        ent, ql_ref[...], (((1,), (1,)), ((), ())), preferred_element_type=jnp.float32
    )
    soft = 1.0 / (1.0 + jnp.exp(-sharpness * (score - lvl_ref[...])))
    o_ref[...] += jnp.sum(soft.reshape(-1, 8, queries), axis=0)


def soft_counts(query, level, table):
    queries, width = query.shape
    rows = table.shape[0]
    eb = 512
    out = pl.pallas_call(
        score_kernel,
        grid=(rows // eb,),
        in_specs=[
            pl.BlockSpec((queries, width), lambda i: (0, 0)),
            pl.BlockSpec((1, queries), lambda i: (0, 0)),
            pl.BlockSpec((eb, width), lambda i: (i, 0)),
        ],
        out_specs=pl.BlockSpec((8, queries), lambda i: (0, 0)),
        out_shape=jax.ShapeDtypeStruct((8, queries), jnp.float32),
        scratch_shapes=[pltpu.VMEM((queries, width), jnp.bfloat16)],
        cost_estimate=pl.CostEstimate(
            flops=2 * queries * rows * width,
            transcendentals=2 * queries * rows,
            bytes_accessed=4 * width * (rows + queries),
        ),
        name="soft_counts",
    )(query, level.reshape(1, queries), table)
    return jnp.sum(out, axis=0)


def pick_rows(table, ids, start):
    count = table.shape[0]
    local = ids - start
    owned = (local >= 0) & (local < count)
    picked = jnp.take(table, jnp.clip(local, 0, count - 1), axis=0, mode="clip")
    return jnp.where(owned[:, None], picked, 0.0)


def shards(entity_table, relations, thresholds, head_ids, rel_ids, thr_idx):
    rows, width = entity_table.shape
    devices = lax.axis_size(ALL)
    queries = head_ids.shape[0]
    ents = rows * devices
    me = lax.axis_index(ALL)
    core = lax.axis_index("c")
    swap = [(0, 1), (1, 0)]
    start = me * rows
    home = queries // devices

    sizes = [lax.axis_size(a) for a in ALL]
    order = lambda v: v.reshape(*sizes, home).transpose(2, 0, 1, 3, 4, 5).reshape(2, queries // 2)

    high, z = lax.axis_index("yh"), lax.axis_index("z")
    hop_y = jnp.asarray([h[0] for h in HOPS], jnp.int32)
    hop_z = jnp.asarray([h[1] for h in HOPS], jnp.int32)
    to = (high ^ hop_y) * 4 + (z + hop_z) % 4
    origin = (high ^ hop_y) * 4 + (z - hop_z) % 4

    flat1 = flipped(entity_table, to, *PARTS[0])
    got1 = sent(flat1)

    ids = order(head_ids)
    ids, flat1 = lax.optimization_barrier((ids, flat1))
    theirs = pick_rows(entity_table, jnp.take(ids, 1 - core, axis=0), start)
    passed = lax.ppermute(theirs, "c", swap)
    mine = pick_rows(entity_table, jnp.take(ids, core, axis=0), start) + passed
    part = exchange(mine, "x")
    part = jnp.sum(part.reshape(4, -1, width), axis=0)
    part = exchange(part, YZ)
    head_vecs = jnp.sum(part.reshape(16, home, width), axis=0)

    my_rel = lax.dynamic_slice(rel_ids, (me * home,), (home,))
    query = head_vecs * jnp.take(relations, my_rel, axis=0, mode="clip")

    flat2 = flipped(entity_table, to, *PARTS[1])
    query = spread(query, YZ).reshape(-1, width)
    flat2, got1, query = lax.optimization_barrier((flat2, got1, query))
    got2 = sent(flat2)
    query = spread(query, "x").reshape(-1, width)
    other = lax.ppermute(query, "c", swap)

    hot = thr_idx[:, None] == jnp.arange(thresholds.shape[0])[None, :]
    level = order(jnp.sum(jnp.where(hot, thresholds[None, :], 0.0), axis=1))
    sum_own = soft_counts(query, jnp.take(level, core, axis=0), entity_table)
    sum_other = soft_counts(other, jnp.take(level, 1 - core, axis=0), entity_table)
    pair = jnp.stack([sum_own, sum_other])
    pair = jnp.where(core == 0, pair, pair[::-1])
    share = pair.reshape(2, 4, 2, 2, 4, home).transpose(1, 2, 0, 3, 4, 5).reshape(devices, home)
    got = exchange(share, ALL)
    fraction = jnp.sum(got, axis=0) * (1.0 / ents)

    table = placed(got1, origin, PARTS[0][0], rows, None)
    table = placed(got2, origin, PARTS[1][0], rows, table)
    return (table.T, fraction)


def solution(mesh):
    fine = Mesh(mesh.devices.reshape(4, 2, 2, 2, 4), ALL)
    whole = P(ALL, None)

    return jax.shard_map(
        shards,
        mesh=fine,
        in_specs=(whole, P(), P(), P(), P(), P()),
        out_specs=(P(("x", "yl", "c"), DIM), P(ALL)),
        check_vma=False,
    )
```

```python
import functools

import jax
import jax.numpy as jnp
from jax import lax
from jax.experimental import pallas as pl
from jax.experimental.pallas import tpu as pltpu
from jax.sharding import Mesh
from jax.sharding import PartitionSpec as P


sharpness = 2.0
ALL = ("x", "yl", "c", "yh", "z")
DIM = ("yh", "z")
YZ = ("yl", "yh", "z")
PARTS = ((0, 1024), (1024, 3072))
CAP = 16
BLK = 512


def exchange(value, axis):
    return lax.all_to_all(value, axis, split_axis=0, concat_axis=0, tiled=True)


def spread(value, axis):
    count = lax.axis_size(axis)
    copies = jnp.broadcast_to(value[None], (count,) + value.shape)
    return exchange(copies, axis)


HOPS = tuple((dy, dz) for dz in (0, 1, 3, 2) for dy in (0, 1))


def flip_kernel(to_ref, x_ref, *refs):
    outs, turned = refs[:-1], refs[-1]
    turned[...] = x_ref[...].T
    cols = outs[0].shape[0]
    for k, o_ref in enumerate(outs):
        first = pl.multiple_of(to_ref[k] * cols, cols)
        o_ref[...] = turned[pl.ds(first, cols), :]


def flipped(table, to, start, length):
    width = table.shape[1]
    cols = width // len(HOPS)
    first = start // BLK
    spec = pl.BlockSpec((cols, BLK), lambda i, to: (0, i))
    return pl.pallas_call(
        flip_kernel,
        grid_spec=pltpu.PrefetchScalarGridSpec(
            num_scalar_prefetch=1,
            grid=(length // BLK,),
            in_specs=[pl.BlockSpec((BLK, width), lambda i, to: (first + i, 0))],
            out_specs=[spec] * len(HOPS),
            scratch_shapes=[pltpu.VMEM((width, BLK), table.dtype)],
        ),
        out_shape=[jax.ShapeDtypeStruct((cols, length), table.dtype)] * len(HOPS),
        cost_estimate=pl.CostEstimate(flops=0, transcendentals=0, bytes_accessed=8 * width * length),
        name="flip",
    )(to, table)


def place_kernel(start, rows, from_ref, *refs):
    count = len(HOPS)
    parts, (out, held, sems_in, sems_out) = refs[:count], refs[-4:]
    loads, stores = [], []
    for k, part in enumerate(parts):
        at = pl.multiple_of(from_ref[k] * rows + start, 128)
        loads.append(pltpu.make_async_copy(part, held.at[k], sems_in.at[k]))
        stores.append(
            pltpu.make_async_copy(held.at[k], out.at[:, pl.ds(at, part.shape[1])], sems_out.at[k])
        )
    for load in loads:
        load.start()
    for load, store in zip(loads, stores):
        load.wait()
        store.start()
    for store in stores:
        store.wait()


def placed(parts, origin, start, rows, held):
    count = len(parts)
    cols, length = parts[0].shape
    args = list(parts)
    if held is not None:
        args.append(held)
    return pl.pallas_call(
        functools.partial(place_kernel, start, rows),
        in_specs=[pl.BlockSpec(memory_space=pltpu.SMEM)] + [pl.BlockSpec(memory_space=pl.ANY)] * len(args),
        out_specs=pl.BlockSpec(memory_space=pl.ANY),
        out_shape=jax.ShapeDtypeStruct((cols, count * rows), parts[0].dtype),
        scratch_shapes=[
            pltpu.VMEM((count, cols, length), parts[0].dtype),
            pltpu.SemaphoreType.DMA((count,)),
            pltpu.SemaphoreType.DMA((count,)),
        ],
        input_output_aliases={} if held is None else {count + 1: 0},
        name="place",
    )(origin, *args)


def sent(parts):
    got = [parts[0]]
    for (dy, dz), part in list(zip(HOPS, parts))[1:]:
        way = [(y * 4 + z, (y ^ dy) * 4 + (z + dz) % 4) for y in range(2) for z in range(4)]
        got.append(lax.ppermute(part, DIM, way))
    return got


def score_kernel(q_ref, lvl_ref, e_ref, o_ref, ql_ref):
    queries = q_ref.shape[0]

    @pl.when(pl.program_id(0) == 0)
    def _():
        ql_ref[...] = q_ref[...].astype(jnp.bfloat16)
        o_ref[...] = jnp.zeros_like(o_ref)

    ent = e_ref[...].astype(jnp.bfloat16)
    score = lax.dot_general(
        ent, ql_ref[...], (((1,), (1,)), ((), ())), preferred_element_type=jnp.float32
    )
    soft = 1.0 / (1.0 + jnp.exp(-sharpness * (score - lvl_ref[...])))
    o_ref[...] += jnp.sum(soft.reshape(-1, 8, queries), axis=0)


def soft_counts(query, level, table):
    queries, width = query.shape
    rows = table.shape[0]
    eb = 512
    out = pl.pallas_call(
        score_kernel,
        grid=(rows // eb,),
        in_specs=[
            pl.BlockSpec((queries, width), lambda i: (0, 0)),
            pl.BlockSpec((1, queries), lambda i: (0, 0)),
            pl.BlockSpec((eb, width), lambda i: (i, 0)),
        ],
        out_specs=pl.BlockSpec((8, queries), lambda i: (0, 0)),
        out_shape=jax.ShapeDtypeStruct((8, queries), jnp.float32),
        scratch_shapes=[pltpu.VMEM((queries, width), jnp.bfloat16)],
        cost_estimate=pl.CostEstimate(
            flops=2 * queries * rows * width,
            transcendentals=2 * queries * rows,
            bytes_accessed=4 * width * (rows + queries),
        ),
        name="soft_counts",
    )(query, level.reshape(1, queries), table)
    return jnp.sum(out, axis=0)


def pick_rows(table, ids, start):
    count = table.shape[0]
    local = ids - start
    owned = (local >= 0) & (local < count)
    picked = jnp.take(table, jnp.clip(local, 0, count - 1), axis=0, mode="clip")
    return jnp.where(owned[:, None], picked, 0.0)


def shards(entity_table, relations, thresholds, head_ids, rel_ids, thr_idx):
    rows, width = entity_table.shape
    devices = lax.axis_size(ALL)
    queries = head_ids.shape[0]
    ents = rows * devices
    me = lax.axis_index(ALL)
    core = lax.axis_index("c")
    swap = [(0, 1), (1, 0)]
    start = me * rows
    home = queries // devices

    sizes = [lax.axis_size(a) for a in ALL]
    order = lambda v: v.reshape(*sizes, home).transpose(2, 0, 1, 3, 4, 5).reshape(2, queries // 2)

    high, z = lax.axis_index("yh"), lax.axis_index("z")
    hop_y = jnp.asarray([h[0] for h in HOPS], jnp.int32)
    hop_z = jnp.asarray([h[1] for h in HOPS], jnp.int32)
    to = (high ^ hop_y) * 4 + (z + hop_z) % 4
    origin = (high ^ hop_y) * 4 + (z - hop_z) % 4

    classes = lambda v: v.reshape(*sizes, home).transpose(1, 3, 4, 0, 2, 5).reshape(16, queries // 16)
    ids = classes(head_ids)
    owner = ids // rows
    local = ids - owner * rows
    spot = jnp.arange(queries // 16)
    same = owner[:, :, None] == owner[:, None, :]
    rank = jnp.sum((same & (spot[None, None, :] < spot[None, :, None])).astype(jnp.int32), axis=2)
    fits = jnp.max(rank) < CAP
    slot = jnp.arange(CAP)
    hit = (owner == me)[:, None, :] & (rank[:, None, :] == slot[None, :, None])
    wanted = jnp.sum(jnp.where(hit, local[:, None, :], 0), axis=2).reshape(-1)
    out_rows = jnp.take(entity_table, wanted, axis=0, mode="clip").reshape(16, CAP, width)
    found = exchange(out_rows, YZ).reshape(-1, width)
    flat1 = flipped(entity_table, to, *PARTS[0])
    got1 = sent(flat1)
    my_class = lax.axis_index(YZ)
    my_owner = jnp.take(owner, my_class, axis=0)
    my_rank = jnp.take(rank, my_class, axis=0)
    mine = (my_owner // 32 == lax.axis_index("x")) & ((my_owner // 8) % 2 == core)
    source = (my_owner // 16) % 2 * 8 + my_owner % 8
    at = jnp.where(mine, source * CAP + my_rank, 0)
    part = jnp.where(mine[:, None], jnp.take(found, at, axis=0, mode="clip"), 0.0)
    part = exchange(part.reshape(8, home, width), ("x", "c"))
    head_vecs = jnp.sum(part, axis=0)

    def every_row(unused):
        full = pick_rows(entity_table, head_ids, start)
        full = exchange(full.reshape(devices, home, width), ALL)
        return jnp.sum(full, axis=0)

    head_vecs = lax.cond(fits, lambda h: h, every_row, head_vecs)
    my_rel = lax.dynamic_slice(rel_ids, (me * home,), (home,))
    query = head_vecs * jnp.take(relations, my_rel, axis=0, mode="clip")

    flat2 = flipped(entity_table, to, *PARTS[1])
    query = spread(query, YZ).reshape(-1, width)
    got2 = sent(flat2)
    query = spread(query, "x").reshape(-1, width)
    other = lax.ppermute(query, "c", swap)

    hot = thr_idx[:, None] == jnp.arange(thresholds.shape[0])[None, :]
    level = order(jnp.sum(jnp.where(hot, thresholds[None, :], 0.0), axis=1))
    sum_own = soft_counts(query, jnp.take(level, core, axis=0), entity_table)
    sum_other = soft_counts(other, jnp.take(level, 1 - core, axis=0), entity_table)
    pair = jnp.stack([sum_own, sum_other])
    pair = jnp.where(core == 0, pair, pair[::-1])
    share = pair.reshape(2, 4, 2, 2, 4, home).transpose(1, 2, 0, 3, 4, 5).reshape(devices, home)
    got = exchange(share, ALL)
    fraction = jnp.sum(got, axis=0) * (1.0 / ents)

    table = placed(got1, origin, PARTS[0][0], rows, None)
    table = placed(got2, origin, PARTS[1][0], rows, table)
    return (table.T, fraction)


def solution(mesh):
    fine = Mesh(mesh.devices.reshape(4, 2, 2, 2, 4), ALL)
    whole = P(ALL, None)

    return jax.shard_map(
        shards,
        mesh=fine,
        in_specs=(whole, P(), P(), P(), P(), P()),
        out_specs=(P(("x", "yl", "c"), DIM), P(ALL)),
        check_vma=False,
    )
```

```python
import functools

import jax
import jax.numpy as jnp
from jax import lax
from jax.experimental import pallas as pl
from jax.experimental.pallas import tpu as pltpu
from jax.sharding import Mesh
from jax.sharding import PartitionSpec as P


sharpness = 2.0
ALL = ("x", "yl", "c", "yh", "z")
DIM = ("yh", "z")
YZ = ("yl", "yh", "z")
PARTS = ((0, 1536), (1536, 2560))
CAP = 16
BLK = 512


def exchange(value, axis):
    return lax.all_to_all(value, axis, split_axis=0, concat_axis=0, tiled=True)


def spread(value, axis):
    count = lax.axis_size(axis)
    copies = jnp.broadcast_to(value[None], (count,) + value.shape)
    return exchange(copies, axis)


HOPS = ((0, 0), (1, 0), (0, 1), (0, 3), (1, 2), (1, 1), (1, 3), (0, 2))
GROUPS = ((0, 1, 2, 3), (4, 5), (6, 7))


def flip_kernel(to_ref, x_ref, *refs):
    outs, turned = refs[:-1], refs[-1]
    turned[...] = x_ref[...].T
    cols = outs[0].shape[0]
    for k, o_ref in enumerate(outs):
        first = pl.multiple_of(to_ref[k] * cols, cols)
        o_ref[...] = turned[pl.ds(first, cols), :]


def flipped(table, to, start, length):
    width = table.shape[1]
    cols = width // len(HOPS)
    first = start // BLK
    spec = pl.BlockSpec((cols, BLK), lambda i, to: (0, i))
    return pl.pallas_call(
        flip_kernel,
        grid_spec=pltpu.PrefetchScalarGridSpec(
            num_scalar_prefetch=1,
            grid=(length // BLK,),
            in_specs=[pl.BlockSpec((BLK, width), lambda i, to: (first + i, 0))],
            out_specs=[spec] * len(HOPS),
            scratch_shapes=[pltpu.VMEM((width, BLK), table.dtype)],
        ),
        out_shape=[jax.ShapeDtypeStruct((cols, length), table.dtype)] * len(HOPS),
        cost_estimate=pl.CostEstimate(flops=0, transcendentals=0, bytes_accessed=8 * width * length),
        name="flip",
    )(to, table)


def place_kernel(start, rows, hops, from_ref, *refs):
    count = len(hops)
    parts, (out, held, sems_in, sems_out) = refs[:count], refs[-4:]
    loads, stores = [], []
    for k, part in enumerate(parts):
        at = pl.multiple_of(from_ref[hops[k]] * rows + start, 128)
        loads.append(pltpu.make_async_copy(part, held.at[k], sems_in.at[k]))
        stores.append(
            pltpu.make_async_copy(held.at[k], out.at[:, pl.ds(at, part.shape[1])], sems_out.at[k])
        )
    for load in loads:
        load.start()
    for load, store in zip(loads, stores):
        load.wait()
        store.start()
    for store in stores:
        store.wait()


def placed(parts, origin, hops, start, rows, held):
    count = len(hops)
    cols, length = parts[0].shape
    args = [parts[k] for k in hops]
    if held is not None:
        args.append(held)
    return pl.pallas_call(
        functools.partial(place_kernel, start, rows, hops),
        in_specs=[pl.BlockSpec(memory_space=pltpu.SMEM)] + [pl.BlockSpec(memory_space=pl.ANY)] * len(args),
        out_specs=pl.BlockSpec(memory_space=pl.ANY),
        out_shape=jax.ShapeDtypeStruct((cols, len(HOPS) * rows), parts[0].dtype),
        scratch_shapes=[
            pltpu.VMEM((count, cols, length), parts[0].dtype),
            pltpu.SemaphoreType.DMA((count,)),
            pltpu.SemaphoreType.DMA((count,)),
        ],
        input_output_aliases={} if held is None else {count + 1: 0},
        name="place",
    )(origin, *args)


def hopped(part, hop):
    dy, dz = hop
    way = [(y * 4 + z, (y ^ dy) * 4 + (z + dz) % 4) for y in range(2) for z in range(4)]
    return lax.ppermute(part, DIM, way)


def score_kernel(*refs):
    q_refs, (lvl_ref, e_ref, o_ref, ql_ref, acc_ref) = refs[:-5], refs[-5:]
    queries = ql_ref.shape[0]
    piece = queries // len(q_refs)
    step = pl.program_id(0)

    @pl.when(step == 0)
    def _():
        for k, q_ref in enumerate(q_refs):
            ql_ref[k * piece : (k + 1) * piece, :] = q_ref[...].astype(jnp.bfloat16)
        acc_ref[...] = jnp.zeros_like(acc_ref)

    ent = e_ref[...].astype(jnp.bfloat16)
    score = lax.dot_general(
        ent, ql_ref[...], (((1,), (1,)), ((), ())), preferred_element_type=jnp.float32
    )
    soft = 1.0 / (1.0 + jnp.exp(-sharpness * (score - lvl_ref[...])))
    acc_ref[...] += jnp.sum(soft.reshape(-1, 8, queries), axis=0)

    @pl.when(step == pl.num_programs(0) - 1)
    def _():
        o_ref[...] = jnp.sum(acc_ref[...], axis=0, keepdims=True)


def soft_counts(pieces, level, table):
    piece, width = pieces[0].shape
    queries = piece * len(pieces)
    rows = table.shape[0]
    eb = 512
    return pl.pallas_call(
        score_kernel,
        grid=(rows // eb,),
        in_specs=[pl.BlockSpec((piece, width), lambda i: (0, 0))] * len(pieces)
        + [
            pl.BlockSpec((1, queries), lambda i: (0, 0)),
            pl.BlockSpec((eb, width), lambda i: (i, 0)),
        ],
        out_specs=pl.BlockSpec((1, queries), lambda i: (0, 0)),
        out_shape=jax.ShapeDtypeStruct((1, queries), jnp.float32),
        scratch_shapes=[
            pltpu.VMEM((queries, width), jnp.bfloat16),
            pltpu.VMEM((8, queries), jnp.float32),
        ],
        cost_estimate=pl.CostEstimate(
            flops=2 * queries * rows * width,
            transcendentals=2 * queries * rows,
            bytes_accessed=4 * width * (rows + queries),
        ),
        name="soft_counts",
    )(*pieces, level.reshape(1, queries), table)


def pick_rows(table, ids, start):
    count = table.shape[0]
    local = ids - start
    owned = (local >= 0) & (local < count)
    picked = jnp.take(table, jnp.clip(local, 0, count - 1), axis=0, mode="clip")
    return jnp.where(owned[:, None], picked, 0.0)


def shards(entity_table, relations, thresholds, head_ids, rel_ids, thr_idx):
    rows, width = entity_table.shape
    devices = lax.axis_size(ALL)
    queries = head_ids.shape[0]
    ents = rows * devices
    me = lax.axis_index(ALL)
    core = lax.axis_index("c")
    swap = [(0, 1), (1, 0)]
    start = me * rows
    home = queries // devices

    sizes = [lax.axis_size(a) for a in ALL]
    x = lax.axis_index("x")
    classes = lambda v: v.reshape(*sizes, home).transpose(0, 2, 1, 3, 4, 5).reshape(8, queries // 8)
    high, z = lax.axis_index("yh"), lax.axis_index("z")
    hop_y = jnp.asarray([h[0] for h in HOPS], jnp.int32)
    hop_z = jnp.asarray([h[1] for h in HOPS], jnp.int32)
    to = (high ^ hop_y) * 4 + (z + hop_z) % 4
    origin = (high ^ hop_y) * 4 + (z - hop_z) % 4

    flat1 = flipped(entity_table, to, *PARTS[0])
    got1 = [flat1[0]] + [hopped(p, h) for p, h in zip(flat1[1:], HOPS[1:])]

    ids = classes(head_ids)
    owner = ids // rows
    local = ids - owner * rows
    spot = jnp.arange(queries // 8)
    same = owner[:, :, None] == owner[:, None, :]
    rank = jnp.sum((same & (spot[None, None, :] < spot[None, :, None])).astype(jnp.int32), axis=2)
    fits = jnp.max(rank) < CAP
    slot = jnp.arange(CAP)
    hit = (owner == me)[:, None, :] & (rank[:, None, :] == slot[None, :, None])
    wanted = jnp.sum(jnp.where(hit, local[:, None, :], 0), axis=2).reshape(-1)
    out_rows = jnp.take(entity_table, wanted, axis=0, mode="clip").reshape(8, CAP, width)
    found = exchange(out_rows, ("x", "c")).reshape(-1, width)
    my_class = x * 2 + core
    my_owner = jnp.take(owner, my_class, axis=0)
    my_rank = jnp.take(rank, my_class, axis=0)
    mine = ((my_owner // 16) % 2 == lax.axis_index("yl")) & (my_owner % 8 == lax.axis_index(DIM))
    source = my_owner // 32 * 2 + (my_owner // 8) % 2
    at = jnp.where(mine, source * CAP + my_rank, 0)
    part = jnp.where(mine[:, None], jnp.take(found, at, axis=0, mode="clip"), 0.0)
    part = exchange(part.reshape(16, home, width), YZ)
    head_vecs = jnp.sum(part, axis=0)

    def every_row(unused):
        full = pick_rows(entity_table, head_ids, start)
        full = exchange(full.reshape(devices, home, width), ALL)
        return jnp.sum(full, axis=0)

    head_vecs = lax.cond(fits, lambda h: h, every_row, head_vecs)
    my_rel = lax.dynamic_slice(rel_ids, (me * home,), (home,))
    query = head_vecs * jnp.take(relations, my_rel, axis=0, mode="clip")

    flat2 = flipped(entity_table, to, *PARTS[1])
    query = spread(query, YZ).reshape(-1, width)
    got2 = [flat2[0]] + [hopped(p, h) for p, h in zip(flat2[1:5], HOPS[1:5])]
    blocks = [query]
    for shift in (1, 3, 2):
        blocks.append(lax.ppermute(query, "x", [(i, (i + shift) % 4) for i in range(4)]))
    got2 += [hopped(p, h) for p, h in zip(flat2[5:], HOPS[5:])]
    others = [lax.ppermute(b, "c", swap) for b in blocks]

    hot = thr_idx[:, None] == jnp.arange(thresholds.shape[0])[None, :]
    level = classes(jnp.sum(jnp.where(hot, thresholds[None, :], 0.0), axis=1))
    turn = jnp.asarray([0, 0, 1, 3, 1, 3, 2, 2], jnp.int32)
    side = jnp.asarray([0, 1, 0, 0, 1, 1, 0, 1], jnp.int32)
    level = jnp.take(level, (x - turn) % 4 * 2 + (core ^ side), axis=0)
    calls = (
        ([blocks[0]], level[0]),
        ([others[0]], level[1]),
        (blocks[1:3], level[2:4]),
        (others[1:3], level[4:6]),
        ([blocks[3], others[3]], level[6:8]),
    )
    sums = [soft_counts(q, lv, entity_table) for q, lv in calls]
    sums = jnp.concatenate(sums, axis=1).reshape(8, queries // 8)
    place = jnp.asarray([0, 1, 2, 4, 6, 7, 3, 5], jnp.int32)
    spin = (x - jnp.arange(4)[:, None]) % 4 * 2 + (core ^ jnp.arange(2)[None, :])
    sums = jnp.take(sums, jnp.take(place, spin.reshape(8)), axis=0)
    got = exchange(sums.reshape(devices, home), ("x", "c", "yl", "yh", "z"))
    fraction = jnp.sum(got, axis=0) * (1.0 / ents)

    table = placed(got1, origin, tuple(range(8)), PARTS[0][0], rows, None)
    for group in GROUPS:
        table = placed(got2, origin, group, PARTS[1][0], rows, table)
    return (table.T, fraction)


def solution(mesh):
    fine = Mesh(mesh.devices.reshape(4, 2, 2, 2, 4), ALL)
    whole = P(ALL, None)

    return jax.shard_map(
        shards,
        mesh=fine,
        in_specs=(whole, P(), P(), P(), P(), P()),
        out_specs=(P(("x", "yl", "c"), DIM), P(ALL)),
        check_vma=False,
    )
```

```python
import functools

import jax
import jax.numpy as jnp
from jax import lax
from jax.experimental import pallas as pl
from jax.experimental.pallas import tpu as pltpu
from jax.sharding import Mesh
from jax.sharding import PartitionSpec as P


sharpness = 2.0
ALL = ("x", "yl", "c", "yh", "z")
DIM = ("yh", "z")
YZ = ("yl", "yh", "z")
PARTS = ((0, 1536), (1536, 2560))
CAP = 16
CAP_YZ = 40
BLK = 256
SPLIT = 4
STEP = 1024
SUB = 512
SHIFTS = (0, 1, 3, 2)


def exchange(value, axis):
    return lax.all_to_all(value, axis, split_axis=0, concat_axis=0, tiled=True)


def spread(value, axis):
    count = lax.axis_size(axis)
    copies = jnp.broadcast_to(value[None], (count,) + value.shape)
    return exchange(copies, axis)


HOPS = ((0, 0), (1, 0), (0, 1), (0, 3), (1, 2), (1, 1), (1, 3), (0, 2))


def slab_to(hop):
    return (lax.axis_index("yh") ^ hop[0]) * 4 + lax.rem(lax.axis_index("z") + hop[1], 4)


def slab_from(hop):
    return (lax.axis_index("yh") ^ hop[0]) * 4 + lax.rem(lax.axis_index("z") + 4 - hop[1], 4)


def flip_kernel(x_ref, *refs):
    outs, turned = refs[:-1], refs[-1]
    turned[...] = x_ref[...].T
    cols = outs[0].shape[0]
    for hop, o_ref in zip(HOPS, outs):
        first = pl.multiple_of(slab_to(hop) * cols, cols)
        o_ref[...] = turned[pl.ds(first, cols), :]


def flipped(table, start, length):
    width = table.shape[1]
    cols = width // len(HOPS)
    first = start // BLK
    return pl.pallas_call(
        flip_kernel,
        grid=(length // BLK,),
        in_specs=[pl.BlockSpec((BLK, width), lambda i: (first + i, 0))],
        out_specs=[pl.BlockSpec((cols, BLK), lambda i: (0, i))] * len(HOPS),
        scratch_shapes=[pltpu.VMEM((width, BLK), table.dtype)],
        out_shape=[jax.ShapeDtypeStruct((cols, length), table.dtype)] * len(HOPS),
        cost_estimate=pl.CostEstimate(flops=0, transcendentals=0, bytes_accessed=8 * width * length),
        name="flip",
    )(table)


def place_kernel(start, rows, hops, *refs):
    count = len(hops)
    parts, (out, held, sems_in, sems_out) = refs[:count], refs[-4:]
    loads, stores = [], []
    for k, part in enumerate(parts):
        at = pl.multiple_of(slab_from(HOPS[hops[k]]) * rows + start, 128)
        loads.append(pltpu.make_async_copy(part, held.at[k], sems_in.at[k]))
        stores.append(
            pltpu.make_async_copy(held.at[k], out.at[:, pl.ds(at, part.shape[1])], sems_out.at[k])
        )
    for load in loads:
        load.start()
    for load, store in zip(loads, stores):
        load.wait()
        store.start()
    for store in stores:
        store.wait()


def placed(parts, hops, start, rows, held):
    count = len(hops)
    cols, length = parts[0].shape
    args = [parts[k] for k in hops]
    if held is not None:
        args.append(held)
    return pl.pallas_call(
        functools.partial(place_kernel, start, rows, hops),
        in_specs=[pl.BlockSpec(memory_space=pl.ANY)] * len(args),
        out_specs=pl.BlockSpec(memory_space=pl.ANY),
        out_shape=jax.ShapeDtypeStruct((cols, len(HOPS) * rows), parts[0].dtype),
        scratch_shapes=[
            pltpu.VMEM((count, cols, length), parts[0].dtype),
            pltpu.SemaphoreType.DMA((count,)),
            pltpu.SemaphoreType.DMA((count,)),
        ],
        input_output_aliases={} if held is None else {count: 0},
        name="place",
    )(*args)


def hopped(part, hop):
    dy, dz = hop
    way = [(y * 4 + z, (y ^ dy) * 4 + (z + dz) % 4) for y in range(2) for z in range(4)]
    return lax.ppermute(part, DIM, way)


def block_class(block):
    shift, side = block
    return lax.rem(lax.axis_index("x") + 4 - shift, 4) * 2 + (lax.axis_index("c") ^ side)


def score_kernel(blocks, *refs):
    count = len(blocks)
    q_refs, e_refs, (lvl_ref, old_ref, o_ref, ql_ref, row_ref, acc_ref, ent_ref) = (
        refs[:count],
        refs[count : count + SPLIT],
        refs[count + SPLIT :],
    )
    queries = ql_ref.shape[0]
    piece = queries // count
    step = pl.program_id(0)

    @pl.when(step == 0)
    def _():
        for k, block in enumerate(blocks):
            ql_ref[k * piece : (k + 1) * piece, :] = q_refs[k][...].astype(jnp.bfloat16)
            row_ref[:, k * piece : (k + 1) * piece] = lvl_ref[pl.ds(block_class(block), 1), :]
        acc_ref[...] = jnp.zeros_like(acc_ref)

    for k, e_ref in enumerate(e_refs):
        span = e_ref.shape[0]
        ent_ref[k * span : (k + 1) * span, :] = e_ref[...].astype(jnp.bfloat16)
    for first in range(0, STEP, SUB):
        score = lax.dot_general(
            ent_ref[first : first + SUB, :],
            ql_ref[...],
            (((1,), (1,)), ((), ())),
            preferred_element_type=jnp.float32,
        )
        soft = 1.0 / (1.0 + jnp.exp(-sharpness * (score - row_ref[...])))
        acc_ref[...] += jnp.sum(soft.reshape(-1, 8, queries), axis=0)

    @pl.when(step == pl.num_programs(0) - 1)
    def _():
        o_ref[...] = old_ref[...]
        for k, block in enumerate(blocks):
            total = jnp.sum(acc_ref[:, k * piece : (k + 1) * piece], axis=0, keepdims=True)
            o_ref[pl.ds(block_class(block), 1), :] = total


def soft_counts(blocks, pieces, table, level, old):
    piece, width = pieces[0].shape
    queries = piece * len(pieces)
    rows = table.shape[0]
    eb = STEP // SPLIT
    whole = pl.BlockSpec(level.shape, lambda i: (0, 0))
    return pl.pallas_call(
        functools.partial(score_kernel, blocks),
        grid=(rows // STEP,),
        in_specs=[pl.BlockSpec((piece, width), lambda i: (0, 0))] * len(pieces)
        + [pl.BlockSpec((eb, width), lambda i, j=j: (i * SPLIT + j, 0)) for j in range(SPLIT)]
        + [whole, whole],
        out_specs=whole,
        out_shape=jax.ShapeDtypeStruct(old.shape, jnp.float32),
        scratch_shapes=[
            pltpu.VMEM((queries, width), jnp.bfloat16),
            pltpu.VMEM((1, queries), jnp.float32),
            pltpu.VMEM((8, queries), jnp.float32),
            pltpu.VMEM((STEP, width), jnp.bfloat16),
        ],
        cost_estimate=pl.CostEstimate(
            flops=2 * queries * rows * width,
            transcendentals=2 * queries * rows,
            bytes_accessed=4 * width * (rows + queries),
        ),
        name="soft_counts",
    )(*pieces, *([table] * SPLIT), level, old)


def pick_rows(table, ids, start):
    count = table.shape[0]
    local = ids - start
    owned = (local >= 0) & (local < count)
    picked = jnp.take(table, jnp.clip(local, 0, count - 1), axis=0, mode="clip")
    return jnp.where(owned[:, None], picked, 0.0)


def shards(entity_table, relations, thresholds, head_ids, rel_ids, thr_idx):
    rows, width = entity_table.shape
    devices = lax.axis_size(ALL)
    queries = head_ids.shape[0]
    ents = rows * devices
    me = lax.axis_index(ALL)
    core = lax.axis_index("c")
    swap = [(0, 1), (1, 0)]
    start = me * rows
    home = queries // devices

    sizes = [lax.axis_size(a) for a in ALL]
    x = lax.axis_index("x")
    classes = lambda v: v.reshape(*sizes, home).transpose(0, 2, 1, 3, 4, 5).reshape(8, queries // 8)
    flat1 = flipped(entity_table, *PARTS[0])
    got1 = [flat1[0]] + [hopped(p, h) for p, h in zip(flat1[1:5], HOPS[1:5])]

    ids = classes(head_ids)
    owner = ids // rows
    local = ids - owner * rows
    members = queries // 8
    spot = jnp.arange(members)
    earlier = spot[None, None, :] < spot[None, :, None]

    def rank_of(key):
        same = key[:, :, None] == key[:, None, :]
        return jnp.sum((same & earlier).astype(jnp.int32), axis=2)

    rank = rank_of(owner)
    slot = jnp.arange(CAP)
    hit = (owner == me)[:, None, :] & (rank[:, None, :] == slot[None, :, None])
    wanted = jnp.sum(jnp.where(hit, local[:, None, :], 0), axis=2).reshape(-1)
    out_rows = jnp.take(entity_table, wanted, axis=0, mode="clip").reshape(8, CAP, width)
    found = exchange(out_rows, ("x", "c")).reshape(-1, width)
    got1 += [hopped(p, h) for p, h in zip(flat1[5:], HOPS[5:])]

    plane = (owner // 16) % 2 * 8 + owner % 8
    plane_rank = rank_of(plane)
    fits = (jnp.max(rank) < CAP) & (jnp.max(plane_rank) < CAP_YZ)
    source = owner // 32 * 2 + (owner // 8) % 2
    stack = jnp.stack([plane, plane_rank, source * CAP + rank, classes(rel_ids)])
    my_plane, my_rank, my_spot, my_rel = jnp.take(stack, x * 2 + core, axis=1)
    place = jnp.arange(CAP_YZ)[:, None]
    chosen = (my_plane == lax.axis_index(YZ))[None, :] & (my_rank[None, :] == place)
    from_spot = jnp.sum(jnp.where(chosen, my_spot[None, :], 0), axis=1)
    from_rel = jnp.sum(jnp.where(chosen, my_rel[None, :], 0), axis=1)
    back = my_plane * CAP_YZ + my_rank
    factor = jnp.take(relations, from_rel, axis=0, mode="clip")
    sent_rows = jnp.take(found, from_spot, axis=0, mode="clip") * factor

    def every_row(unused):
        full = pick_rows(entity_table, head_ids, start)
        full = exchange(full.reshape(devices, home, width), ALL)
        one_rel = lax.dynamic_slice(rel_ids, (me * home,), (home,))
        one = jnp.sum(full, axis=0) * jnp.take(relations, one_rel, axis=0, mode="clip")
        return spread(one, YZ).reshape(-1, width)

    flat2 = flipped(entity_table, *PARTS[1])
    query = spread(sent_rows, YZ).reshape(-1, width)
    query = jnp.take(query, back, axis=0, mode="clip")
    query = lax.cond(fits, lambda q: q, every_row, query)
    got2 = [flat2[0]] + [hopped(p, h) for p, h in zip(flat2[1:5], HOPS[1:5])]
    held = {(0, 0): query}
    for shift in SHIFTS[1:]:
        held[shift, 0] = lax.ppermute(query, "x", [(i, (i + shift) % 4) for i in range(4)])
    got2 += [hopped(p, h) for p, h in zip(flat2[5:], HOPS[5:])]
    for shift in SHIFTS:
        held[shift, 1] = lax.ppermute(held[shift, 0], "c", swap)

    hot = classes(thr_idx)[:, :, None] == jnp.arange(thresholds.shape[0])[None, None, :]
    level = jnp.sum(jnp.where(hot, thresholds[None, None, :], 0.0), axis=2)
    sums = jnp.zeros_like(level)
    for shifts in (SHIFTS[:1], SHIFTS[1:]):
        blocks = tuple((shift, side) for side in (0, 1) for shift in shifts)
        sums = soft_counts(blocks, [held[b] for b in blocks], entity_table, level, sums)
    got = exchange(sums.reshape(devices, home), ("x", "c", "yl", "yh", "z"))
    fraction = jnp.sum(got, axis=0) * (1.0 / ents)

    table = placed(got1, tuple(range(8)), PARTS[0][0], rows, None)
    table = placed(got2, tuple(range(8)), PARTS[1][0], rows, table)
    return (table.T, fraction)


def solution(mesh):
    fine = Mesh(mesh.devices.reshape(4, 2, 2, 2, 4), ALL)
    whole = P(ALL, None)

    return jax.shard_map(
        shards,
        mesh=fine,
        in_specs=(whole, P(), P(), P(), P(), P()),
        out_specs=(P(("x", "yl", "c"), DIM), P(ALL)),
        check_vma=False,
    )
```

```python
import functools

import jax
import jax.numpy as jnp
from jax import lax
from jax.experimental import pallas as pl
from jax.experimental.pallas import tpu as pltpu
from jax.sharding import Mesh
from jax.sharding import PartitionSpec as P


sharpness = 2.0
ALL = ("x", "yl", "c", "yh", "z")
DIM = ("yh", "z")
YZ = ("yl", "yh", "z")
PARTS = ((0, 1536), (1536, 2560))
CAP = 16
CAP_YZ = 40
BLK = 512
SPLIT = 8
STEP = 1024
SUB = 256
SHIFTS = (0, 1, 3, 2)


def exchange(value, axis):
    return lax.all_to_all(value, axis, split_axis=0, concat_axis=0, tiled=True)


def spread(value, axis):
    count = lax.axis_size(axis)
    copies = jnp.broadcast_to(value[None], (count,) + value.shape)
    return exchange(copies, axis)


HOPS = ((0, 0), (1, 0), (0, 1), (0, 3), (1, 2), (1, 1), (1, 3), (0, 2))


def slab_to(hop):
    return (lax.axis_index("yh") ^ hop[0]) * 4 + lax.rem(lax.axis_index("z") + hop[1], 4)


def slab_from(hop):
    return (lax.axis_index("yh") ^ hop[0]) * 4 + lax.rem(lax.axis_index("z") + 4 - hop[1], 4)


def flip_kernel(x_ref, *refs):
    outs, turned = refs[:-1], refs[-1]
    turned[...] = x_ref[...].T
    cols = outs[0].shape[0]
    for hop, o_ref in zip(HOPS, outs):
        first = pl.multiple_of(slab_to(hop) * cols, cols)
        o_ref[...] = turned[pl.ds(first, cols), :]


def flipped(table, start, length):
    width = table.shape[1]
    cols = width // len(HOPS)
    first = start // BLK
    return pl.pallas_call(
        flip_kernel,
        grid=(length // BLK,),
        in_specs=[pl.BlockSpec((BLK, width), lambda i: (first + i, 0))],
        out_specs=[pl.BlockSpec((cols, BLK), lambda i: (0, i))] * len(HOPS),
        scratch_shapes=[pltpu.VMEM((width, BLK), table.dtype)],
        out_shape=[jax.ShapeDtypeStruct((cols, length), table.dtype)] * len(HOPS),
        cost_estimate=pl.CostEstimate(flops=0, transcendentals=0, bytes_accessed=8 * width * length),
        name="flip",
    )(table)


def place_kernel(start, rows, hops, *refs):
    count = len(hops)
    parts, (out, held, sems_in, sems_out) = refs[:count], refs[-4:]
    loads, stores = [], []
    for k, part in enumerate(parts):
        at = pl.multiple_of(slab_from(HOPS[hops[k]]) * rows + start, 128)
        loads.append(pltpu.make_async_copy(part, held.at[k], sems_in.at[k]))
        stores.append(
            pltpu.make_async_copy(held.at[k], out.at[:, pl.ds(at, part.shape[1])], sems_out.at[k])
        )
    for load in loads:
        load.start()
    for load, store in zip(loads, stores):
        load.wait()
        store.start()
    for store in stores:
        store.wait()


def placed(parts, hops, start, rows, held):
    count = len(hops)
    cols, length = parts[0].shape
    args = [parts[k] for k in hops]
    if held is not None:
        args.append(held)
    return pl.pallas_call(
        functools.partial(place_kernel, start, rows, hops),
        in_specs=[pl.BlockSpec(memory_space=pl.ANY)] * len(args),
        out_specs=pl.BlockSpec(memory_space=pl.ANY),
        out_shape=jax.ShapeDtypeStruct((cols, len(HOPS) * rows), parts[0].dtype),
        scratch_shapes=[
            pltpu.VMEM((count, cols, length), parts[0].dtype),
            pltpu.SemaphoreType.DMA((count,)),
            pltpu.SemaphoreType.DMA((count,)),
        ],
        input_output_aliases={} if held is None else {count: 0},
        name="place",
    )(*args)


def hopped(part, hop):
    dy, dz = hop
    way = [(y * 4 + z, (y ^ dy) * 4 + (z + dz) % 4) for y in range(2) for z in range(4)]
    return lax.ppermute(part, DIM, way)


def block_class(block):
    shift, side = block
    return lax.rem(lax.axis_index("x") + 4 - shift, 4) * 2 + (lax.axis_index("c") ^ side)


def score_kernel(blocks, *refs):
    count = len(blocks)
    q_refs, e_refs, (lvl_ref, old_ref, o_ref, ql_ref, row_ref, acc_ref, ent_ref) = (
        refs[:count],
        refs[count : count + SPLIT],
        refs[count + SPLIT :],
    )
    queries = ql_ref.shape[0]
    piece = queries // count
    step = pl.program_id(0)

    @pl.when(step == 0)
    def _():
        for k, block in enumerate(blocks):
            ql_ref[k * piece : (k + 1) * piece, :] = q_refs[k][...].astype(jnp.bfloat16)
            row_ref[:, k * piece : (k + 1) * piece] = lvl_ref[pl.ds(block_class(block), 1), :]
        acc_ref[...] = jnp.zeros_like(acc_ref)

    for k, e_ref in enumerate(e_refs):
        span = e_ref.shape[0]
        ent_ref[k * span : (k + 1) * span, :] = e_ref[...].astype(jnp.bfloat16)
    for first in range(0, STEP, SUB):
        score = lax.dot_general(
            ent_ref[first : first + SUB, :],
            ql_ref[...],
            (((1,), (1,)), ((), ())),
            preferred_element_type=jnp.float32,
        )
        soft = 1.0 / (1.0 + jnp.exp(-sharpness * (score - row_ref[...])))
        acc_ref[...] += jnp.sum(soft.reshape(-1, 8, queries), axis=0)

    @pl.when(step == pl.num_programs(0) - 1)
    def _():
        o_ref[...] = old_ref[...]
        for k, block in enumerate(blocks):
            total = jnp.sum(acc_ref[:, k * piece : (k + 1) * piece], axis=0, keepdims=True)
            o_ref[pl.ds(block_class(block), 1), :] = total


def soft_counts(blocks, pieces, table, level, old):
    piece, width = pieces[0].shape
    queries = piece * len(pieces)
    rows = table.shape[0]
    eb = STEP // SPLIT
    whole = pl.BlockSpec(level.shape, lambda i: (0, 0))
    return pl.pallas_call(
        functools.partial(score_kernel, blocks),
        grid=(rows // STEP,),
        in_specs=[pl.BlockSpec((piece, width), lambda i: (0, 0))] * len(pieces)
        + [pl.BlockSpec((eb, width), lambda i, j=j: (i * SPLIT + j, 0)) for j in range(SPLIT)]
        + [whole, whole],
        out_specs=whole,
        out_shape=jax.ShapeDtypeStruct(old.shape, jnp.float32),
        scratch_shapes=[
            pltpu.VMEM((queries, width), jnp.bfloat16),
            pltpu.VMEM((1, queries), jnp.float32),
            pltpu.VMEM((8, queries), jnp.float32),
            pltpu.VMEM((STEP, width), jnp.bfloat16),
        ],
        cost_estimate=pl.CostEstimate(
            flops=2 * queries * rows * width,
            transcendentals=2 * queries * rows,
            bytes_accessed=4 * width * (rows + queries),
        ),
        name="soft_counts",
    )(*pieces, *([table] * SPLIT), level, old)


def pick_rows(table, ids, start):
    count = table.shape[0]
    local = ids - start
    owned = (local >= 0) & (local < count)
    picked = jnp.take(table, jnp.clip(local, 0, count - 1), axis=0, mode="clip")
    return jnp.where(owned[:, None], picked, 0.0)


def shards(entity_table, relations, thresholds, head_ids, rel_ids, thr_idx):
    rows, width = entity_table.shape
    devices = lax.axis_size(ALL)
    queries = head_ids.shape[0]
    ents = rows * devices
    me = lax.axis_index(ALL)
    core = lax.axis_index("c")
    swap = [(0, 1), (1, 0)]
    start = me * rows
    home = queries // devices

    sizes = [lax.axis_size(a) for a in ALL]
    x = lax.axis_index("x")
    classes = lambda v: v.reshape(*sizes, home).transpose(0, 2, 1, 3, 4, 5).reshape(8, queries // 8)
    flat1 = flipped(entity_table, *PARTS[0])
    got1 = [flat1[0]] + [hopped(p, h) for p, h in zip(flat1[1:7], HOPS[1:7])]

    ids = classes(head_ids)
    owner = ids // rows
    local = ids - owner * rows
    members = queries // 8
    spot = jnp.arange(members)
    earlier = spot[None, None, :] < spot[None, :, None]

    def rank_of(key):
        same = key[:, :, None] == key[:, None, :]
        return jnp.sum((same & earlier).astype(jnp.int32), axis=2)

    rank = rank_of(owner)
    slot = jnp.arange(CAP)
    hit = (owner == me)[:, None, :] & (rank[:, None, :] == slot[None, :, None])
    wanted = jnp.sum(jnp.where(hit, local[:, None, :], 0), axis=2).reshape(-1)
    out_rows = jnp.take(entity_table, wanted, axis=0, mode="clip").reshape(8, CAP, width)
    found = exchange(out_rows, ("x", "c")).reshape(-1, width)
    got1 += [hopped(p, h) for p, h in zip(flat1[7:], HOPS[7:])]

    plane = (owner // 16) % 2 * 8 + owner % 8
    plane_rank = rank_of(plane)
    fits = (jnp.max(rank) < CAP) & (jnp.max(plane_rank) < CAP_YZ)
    source = owner // 32 * 2 + (owner // 8) % 2
    stack = jnp.stack([plane, plane_rank, source * CAP + rank, classes(rel_ids)])
    my_plane, my_rank, my_spot, my_rel = jnp.take(stack, x * 2 + core, axis=1)
    place = jnp.arange(CAP_YZ)[:, None]
    chosen = (my_plane == lax.axis_index(YZ))[None, :] & (my_rank[None, :] == place)
    from_spot = jnp.sum(jnp.where(chosen, my_spot[None, :], 0), axis=1)
    from_rel = jnp.sum(jnp.where(chosen, my_rel[None, :], 0), axis=1)
    back = my_plane * CAP_YZ + my_rank
    factor = jnp.take(relations, from_rel, axis=0, mode="clip")
    sent_rows = jnp.take(found, from_spot, axis=0, mode="clip") * factor

    def every_row(unused):
        full = pick_rows(entity_table, head_ids, start)
        full = exchange(full.reshape(devices, home, width), ALL)
        one_rel = lax.dynamic_slice(rel_ids, (me * home,), (home,))
        one = jnp.sum(full, axis=0) * jnp.take(relations, one_rel, axis=0, mode="clip")
        return spread(one, YZ).reshape(-1, width)

    flat2 = flipped(entity_table, *PARTS[1])
    query = spread(sent_rows, YZ).reshape(-1, width)
    query = jnp.take(query, back, axis=0, mode="clip")
    query = lax.cond(fits, lambda q: q, every_row, query)
    got2 = [flat2[0]] + [hopped(p, h) for p, h in zip(flat2[1:4], HOPS[1:4])]
    held = {(0, 0): query}
    for shift in SHIFTS[1:]:
        held[shift, 0] = lax.ppermute(query, "x", [(i, (i + shift) % 4) for i in range(4)])
    got2 += [hopped(p, h) for p, h in zip(flat2[4:], HOPS[4:])]
    for shift in SHIFTS:
        held[shift, 1] = lax.ppermute(held[shift, 0], "c", swap)

    hot = classes(thr_idx)[:, :, None] == jnp.arange(thresholds.shape[0])[None, None, :]
    level = jnp.sum(jnp.where(hot, thresholds[None, None, :], 0.0), axis=2)
    sums = jnp.zeros_like(level)
    for shifts in (SHIFTS[:1], SHIFTS[1:]):
        blocks = tuple((shift, side) for side in (0, 1) for shift in shifts)
        sums = soft_counts(blocks, [held[b] for b in blocks], entity_table, level, sums)
    got = exchange(sums.reshape(devices, home), ("x", "c", "yl", "yh", "z"))
    fraction = jnp.sum(got, axis=0) * (1.0 / ents)

    table = placed(got1, tuple(range(8)), PARTS[0][0], rows, None)
    table = placed(got2, tuple(range(8)), PARTS[1][0], rows, table)
    return (table.T, fraction)


def solution(mesh):
    fine = Mesh(mesh.devices.reshape(4, 2, 2, 2, 4), ALL)
    whole = P(ALL, None)

    return jax.shard_map(
        shards,
        mesh=fine,
        in_specs=(whole, P(), P(), P(), P(), P()),
        out_specs=(P(("x", "yl", "c"), DIM), P(ALL)),
        check_vma=False,
    )
```

```python
import functools

import jax
import jax.numpy as jnp
from jax import lax
from jax.experimental import pallas as pl
from jax.experimental.pallas import tpu as pltpu
from jax.sharding import Mesh
from jax.sharding import PartitionSpec as P


sharpness = 2.0
ALL = ("x", "yl", "c", "yh", "z")
DIM = ("yh", "z")
YZ = ("yl", "yh", "z")
PARTS = ((0, 1536), (1536, 2560))
CAP = 16
ORDER = (1, 2, 3, 5, 6, 4, 7)
CAP_YZ = 40
BLK = 512
SPLIT = 8
STEP = 1024
SUB = 256
SHIFTS = (0, 1, 3, 2)


def exchange(value, axis):
    return lax.all_to_all(value, axis, split_axis=0, concat_axis=0, tiled=True)


def spread(value, axis):
    count = lax.axis_size(axis)
    copies = jnp.broadcast_to(value[None], (count,) + value.shape)
    return exchange(copies, axis)


HOPS = ((0, 0), (1, 0), (0, 1), (0, 3), (1, 2), (1, 1), (1, 3), (0, 2))


def slab_to(hop):
    return (lax.axis_index("yh") ^ hop[0]) * 4 + lax.rem(lax.axis_index("z") + hop[1], 4)


def slab_from(hop):
    return (lax.axis_index("yh") ^ hop[0]) * 4 + lax.rem(lax.axis_index("z") + 4 - hop[1], 4)


def flip_kernel(x_ref, *refs):
    outs, turned = refs[:-1], refs[-1]
    turned[...] = x_ref[...].T
    cols = outs[0].shape[0]
    for hop, o_ref in zip(HOPS, outs):
        first = pl.multiple_of(slab_to(hop) * cols, cols)
        o_ref[...] = turned[pl.ds(first, cols), :]


def flipped(table, start, length):
    width = table.shape[1]
    cols = width // len(HOPS)
    first = start // BLK
    return pl.pallas_call(
        flip_kernel,
        grid=(length // BLK,),
        in_specs=[pl.BlockSpec((BLK, width), lambda i: (first + i, 0))],
        out_specs=[pl.BlockSpec((cols, BLK), lambda i: (0, i))] * len(HOPS),
        scratch_shapes=[pltpu.VMEM((width, BLK), table.dtype)],
        out_shape=[jax.ShapeDtypeStruct((cols, length), table.dtype)] * len(HOPS),
        cost_estimate=pl.CostEstimate(flops=0, transcendentals=0, bytes_accessed=8 * width * length),
        name="flip",
    )(table)


def place_kernel(spots, rows, *refs):
    count = len(spots)
    parts, (out, *rest) = refs[:count], refs[-count - 3 :]
    held, (sems_in, sems_out) = rest[:count], rest[count:]
    loads, stores = [], []
    for k, ((hop, start), part) in enumerate(zip(spots, parts)):
        at = pl.multiple_of(slab_from(HOPS[hop]) * rows + start, 128)
        loads.append(pltpu.make_async_copy(part, held[k], sems_in.at[k]))
        stores.append(
            pltpu.make_async_copy(held[k], out.at[:, pl.ds(at, part.shape[1])], sems_out.at[k])
        )
    for load in loads:
        load.start()
    for load, store in zip(loads, stores):
        load.wait()
        store.start()
    for store in stores:
        store.wait()


def placed(parts, spots, rows, held):
    count = len(parts)
    cols = parts[0].shape[0]
    args = list(parts)
    if held is not None:
        args.append(held)
    return pl.pallas_call(
        functools.partial(place_kernel, spots, rows),
        in_specs=[pl.BlockSpec(memory_space=pl.ANY)] * len(args),
        out_specs=pl.BlockSpec(memory_space=pl.ANY),
        out_shape=jax.ShapeDtypeStruct((cols, len(HOPS) * rows), parts[0].dtype),
        scratch_shapes=[pltpu.VMEM(part.shape, part.dtype) for part in parts]
        + [pltpu.SemaphoreType.DMA((count,)), pltpu.SemaphoreType.DMA((count,))],
        input_output_aliases={} if held is None else {count: 0},
        name="place",
    )(*args)


def hopped(part, hop):
    dy, dz = hop
    way = [(y * 4 + z, (y ^ dy) * 4 + (z + dz) % 4) for y in range(2) for z in range(4)]
    return lax.ppermute(part, DIM, way)


def block_class(block):
    shift, side = block
    return lax.rem(lax.axis_index("x") + 4 - shift, 4) * 2 + (lax.axis_index("c") ^ side)


def score_kernel(blocks, *refs):
    count = len(blocks)
    q_refs, e_refs, (lvl_ref, old_ref, o_ref, ql_ref, row_ref, acc_ref, ent_ref) = (
        refs[:count],
        refs[count : count + SPLIT],
        refs[count + SPLIT :],
    )
    queries = ql_ref.shape[0]
    piece = queries // count
    step = pl.program_id(0)

    @pl.when(step == 0)
    def _():
        for k, block in enumerate(blocks):
            ql_ref[k * piece : (k + 1) * piece, :] = q_refs[k][...].astype(jnp.bfloat16)
            row_ref[:, k * piece : (k + 1) * piece] = lvl_ref[pl.ds(block_class(block), 1), :]
        acc_ref[...] = jnp.zeros_like(acc_ref)

    for k, e_ref in enumerate(e_refs):
        span = e_ref.shape[0]
        ent_ref[k * span : (k + 1) * span, :] = e_ref[...].astype(jnp.bfloat16)
    for first in range(0, STEP, SUB):
        score = lax.dot_general(
            ent_ref[first : first + SUB, :],
            ql_ref[...],
            (((1,), (1,)), ((), ())),
            preferred_element_type=jnp.float32,
        )
        soft = 1.0 / (1.0 + jnp.exp(-sharpness * (score - row_ref[...])))
        acc_ref[...] += jnp.sum(soft.reshape(-1, 8, queries), axis=0)

    @pl.when(step == pl.num_programs(0) - 1)
    def _():
        o_ref[...] = old_ref[...]
        for k, block in enumerate(blocks):
            total = jnp.sum(acc_ref[:, k * piece : (k + 1) * piece], axis=0, keepdims=True)
            o_ref[pl.ds(block_class(block), 1), :] = total


def soft_counts(blocks, pieces, table, level, old):
    piece, width = pieces[0].shape
    queries = piece * len(pieces)
    rows = table.shape[0]
    eb = STEP // SPLIT
    whole = pl.BlockSpec(level.shape, lambda i: (0, 0))
    return pl.pallas_call(
        functools.partial(score_kernel, blocks),
        grid=(rows // STEP,),
        in_specs=[pl.BlockSpec((piece, width), lambda i: (0, 0))] * len(pieces)
        + [pl.BlockSpec((eb, width), lambda i, j=j: (i * SPLIT + j, 0)) for j in range(SPLIT)]
        + [whole, whole],
        out_specs=whole,
        out_shape=jax.ShapeDtypeStruct(old.shape, jnp.float32),
        scratch_shapes=[
            pltpu.VMEM((queries, width), jnp.bfloat16),
            pltpu.VMEM((1, queries), jnp.float32),
            pltpu.VMEM((8, queries), jnp.float32),
            pltpu.VMEM((STEP, width), jnp.bfloat16),
        ],
        cost_estimate=pl.CostEstimate(
            flops=2 * queries * rows * width,
            transcendentals=2 * queries * rows,
            bytes_accessed=4 * width * (rows + queries),
        ),
        name="soft_counts",
    )(*pieces, *([table] * SPLIT), level, old)


def pick_rows(table, ids, start):
    count = table.shape[0]
    local = ids - start
    owned = (local >= 0) & (local < count)
    picked = jnp.take(table, jnp.clip(local, 0, count - 1), axis=0, mode="clip")
    return jnp.where(owned[:, None], picked, 0.0)


def shards(entity_table, relations, thresholds, head_ids, rel_ids, thr_idx):
    rows, width = entity_table.shape
    devices = lax.axis_size(ALL)
    queries = head_ids.shape[0]
    ents = rows * devices
    me = lax.axis_index(ALL)
    core = lax.axis_index("c")
    swap = [(0, 1), (1, 0)]
    start = me * rows
    home = queries // devices

    sizes = [lax.axis_size(a) for a in ALL]
    x = lax.axis_index("x")
    classes = lambda v: v.reshape(*sizes, home).transpose(0, 2, 1, 3, 4, 5).reshape(8, queries // 8)
    flat1 = flipped(entity_table, *PARTS[0])
    got1 = [flat1[0]] + [hopped(p, h) for p, h in zip(flat1[1:7], HOPS[1:7])]

    ids = classes(head_ids)
    owner = ids // rows
    local = ids - owner * rows
    members = queries // 8
    spot = jnp.arange(members)
    earlier = spot[None, None, :] < spot[None, :, None]

    def rank_of(key):
        same = key[:, :, None] == key[:, None, :]
        return jnp.sum((same & earlier).astype(jnp.int32), axis=2)

    rank = rank_of(owner)
    slot = jnp.arange(CAP)
    hit = (owner == me)[:, None, :] & (rank[:, None, :] == slot[None, :, None])
    wanted = jnp.sum(jnp.where(hit, local[:, None, :], 0), axis=2).reshape(-1)
    out_rows = jnp.take(entity_table, wanted, axis=0, mode="clip").reshape(8, CAP, width)
    found = exchange(out_rows, ("x", "c")).reshape(-1, width)
    got1 += [hopped(p, h) for p, h in zip(flat1[7:], HOPS[7:])]

    plane = (owner // 16) % 2 * 8 + owner % 8
    plane_rank = rank_of(plane)
    fits = (jnp.max(rank) < CAP) & (jnp.max(plane_rank) < CAP_YZ)
    source = owner // 32 * 2 + (owner // 8) % 2
    stack = jnp.stack([plane, plane_rank, source * CAP + rank, classes(rel_ids)])
    my_plane, my_rank, my_spot, my_rel = jnp.take(stack, x * 2 + core, axis=1)
    place = jnp.arange(CAP_YZ)[:, None]
    chosen = (my_plane == lax.axis_index(YZ))[None, :] & (my_rank[None, :] == place)
    from_spot = jnp.sum(jnp.where(chosen, my_spot[None, :], 0), axis=1)
    from_rel = jnp.sum(jnp.where(chosen, my_rel[None, :], 0), axis=1)
    back = my_plane * CAP_YZ + my_rank
    factor = jnp.take(relations, from_rel, axis=0, mode="clip")
    sent_rows = jnp.take(found, from_spot, axis=0, mode="clip") * factor

    def every_row(unused):
        full = pick_rows(entity_table, head_ids, start)
        full = exchange(full.reshape(devices, home, width), ALL)
        one_rel = lax.dynamic_slice(rel_ids, (me * home,), (home,))
        one = jnp.sum(full, axis=0) * jnp.take(relations, one_rel, axis=0, mode="clip")
        return spread(one, YZ).reshape(-1, width)

    flat2 = flipped(entity_table, *PARTS[1])
    query = spread(sent_rows, YZ).reshape(-1, width)
    query = jnp.take(query, back, axis=0, mode="clip")
    query = lax.cond(fits, lambda q: q, every_row, query)
    got2 = [flat2[0]] + [None] * 7
    for k in ORDER[:3]:
        got2[k] = hopped(flat2[k], HOPS[k])
    held = {(0, 0): query}
    for shift in SHIFTS[1:]:
        held[shift, 0] = lax.ppermute(query, "x", [(i, (i + shift) % 4) for i in range(4)])
    for k in ORDER[3:]:
        got2[k] = hopped(flat2[k], HOPS[k])
    for shift in SHIFTS:
        held[shift, 1] = lax.ppermute(held[shift, 0], "c", swap)

    hot = classes(thr_idx)[:, :, None] == jnp.arange(thresholds.shape[0])[None, None, :]
    level = jnp.sum(jnp.where(hot, thresholds[None, None, :], 0.0), axis=2)
    sums = jnp.zeros_like(level)
    for shifts in (SHIFTS[:1], SHIFTS[1:]):
        blocks = tuple((shift, side) for side in (0, 1) for shift in shifts)
        sums = soft_counts(blocks, [held[b] for b in blocks], entity_table, level, sums)
    got = exchange(sums.reshape(devices, home), ("x", "c", "yl", "yh", "z"))
    fraction = jnp.sum(got, axis=0) * (1.0 / ents)

    first, second = PARTS[0][0], PARTS[1][0]
    spots = tuple((k, first) for k in range(8)) + ((0, second),)
    table = placed(got1 + got2[:1], spots, rows, None)
    table = placed(got2[1:], tuple((k, second) for k in range(1, 8)), rows, table)
    return (table.T, fraction)


def solution(mesh):
    fine = Mesh(mesh.devices.reshape(4, 2, 2, 2, 4), ALL)
    whole = P(ALL, None)

    return jax.shard_map(
        shards,
        mesh=fine,
        in_specs=(whole, P(), P(), P(), P(), P()),
        out_specs=(P(("x", "yl", "c"), DIM), P(ALL)),
        check_vma=False,
    )
```

```python
import functools

import jax
import jax.numpy as jnp
from jax import lax
from jax.experimental import pallas as pl
from jax.experimental.pallas import tpu as pltpu
from jax.sharding import Mesh
from jax.sharding import PartitionSpec as P


sharpness = 2.0
ALL = ("x", "yl", "c", "yh", "z")
DIM = ("yh", "z")
YZ = ("yl", "yh", "z")
PARTS = ((0, 1536), (1536, 2560))
CAP = 16
ORDER = (1, 2, 3, 5, 6, 4, 7)
CAP_YZ = 40
BLK = 512
SPLIT = 8
STEP = 1024
SUB = 256
SHIFTS = (0, 1, 3, 2)


def exchange(value, axis):
    return lax.all_to_all(value, axis, split_axis=0, concat_axis=0, tiled=True)


def spread(value, axis):
    count = lax.axis_size(axis)
    copies = jnp.broadcast_to(value[None], (count,) + value.shape)
    return exchange(copies, axis)


HOPS = ((0, 0), (1, 0), (0, 1), (0, 3), (1, 2), (1, 1), (1, 3), (0, 2))


def slab_to(hop):
    return (lax.axis_index("yh") ^ hop[0]) * 4 + lax.rem(lax.axis_index("z") + hop[1], 4)


def slab_from(hop):
    return (lax.axis_index("yh") ^ hop[0]) * 4 + lax.rem(lax.axis_index("z") + 4 - hop[1], 4)


def flip_kernel(x_ref, *refs):
    outs, turned = refs[:-1], refs[-1]
    turned[...] = x_ref[...].T
    cols = outs[0].shape[0]
    for hop, o_ref in zip(HOPS, outs):
        first = pl.multiple_of(slab_to(hop) * cols, cols)
        o_ref[...] = turned[pl.ds(first, cols), :]


def flipped(table, start, length):
    width = table.shape[1]
    cols = width // len(HOPS)
    first = start // BLK
    return pl.pallas_call(
        flip_kernel,
        grid=(length // BLK,),
        in_specs=[pl.BlockSpec((BLK, width), lambda i: (first + i, 0))],
        out_specs=[pl.BlockSpec((cols, BLK), lambda i: (0, i))] * len(HOPS),
        scratch_shapes=[pltpu.VMEM((width, BLK), table.dtype)],
        out_shape=[jax.ShapeDtypeStruct((cols, length), table.dtype)] * len(HOPS),
        cost_estimate=pl.CostEstimate(flops=0, transcendentals=0, bytes_accessed=8 * width * length),
        name="flip",
    )(table)


def place_kernel(spots, rows, *refs):
    count = len(spots)
    parts, (out, *rest) = refs[:count], refs[-count - 3 :]
    held, (sems_in, sems_out) = rest[:count], rest[count:]
    loads, stores = [], []
    for k, ((hop, start), part) in enumerate(zip(spots, parts)):
        at = pl.multiple_of(slab_from(HOPS[hop]) * rows + start, 128)
        loads.append(pltpu.make_async_copy(part, held[k], sems_in.at[k]))
        stores.append(
            pltpu.make_async_copy(held[k], out.at[:, pl.ds(at, part.shape[1])], sems_out.at[k])
        )
    for load in loads:
        load.start()
    for load, store in zip(loads, stores):
        load.wait()
        store.start()
    for store in stores:
        store.wait()


def placed(parts, spots, rows, held):
    count = len(parts)
    cols = parts[0].shape[0]
    args = list(parts)
    if held is not None:
        args.append(held)
    return pl.pallas_call(
        functools.partial(place_kernel, spots, rows),
        in_specs=[pl.BlockSpec(memory_space=pl.ANY)] * len(args),
        out_specs=pl.BlockSpec(memory_space=pl.ANY),
        out_shape=jax.ShapeDtypeStruct((cols, len(HOPS) * rows), parts[0].dtype),
        scratch_shapes=[pltpu.VMEM(part.shape, part.dtype) for part in parts]
        + [pltpu.SemaphoreType.DMA((count,)), pltpu.SemaphoreType.DMA((count,))],
        input_output_aliases={} if held is None else {count: 0},
        name="place",
    )(*args)


def hopped(part, hop):
    dy, dz = hop
    way = [(y * 4 + z, (y ^ dy) * 4 + (z + dz) % 4) for y in range(2) for z in range(4)]
    return lax.ppermute(part, DIM, way)


def block_class(block):
    shift, side = block
    return lax.rem(lax.axis_index("x") + 4 - shift, 4) * 2 + (lax.axis_index("c") ^ side)


def score_kernel(blocks, weight, *refs):
    count = len(blocks)
    q_refs, e_refs, (lvl_ref, old_ref, o_ref, ql_ref, row_ref, acc_ref, ent_ref) = (
        refs[:count],
        refs[count : count + SPLIT],
        refs[count + SPLIT :],
    )
    queries = ql_ref.shape[0]
    piece = queries // count
    step = pl.program_id(0)

    @pl.when(step == 0)
    def _():
        for k, block in enumerate(blocks):
            ql_ref[k * piece : (k + 1) * piece, :] = q_refs[k][...].astype(jnp.bfloat16)
            row_ref[:, k * piece : (k + 1) * piece] = lvl_ref[pl.ds(block_class(block), 1), :]
        acc_ref[...] = jnp.zeros_like(acc_ref)

    for k, e_ref in enumerate(e_refs):
        span = e_ref.shape[0]
        ent_ref[k * span : (k + 1) * span, :] = e_ref[...].astype(jnp.bfloat16)
    for first in range(0, STEP, SUB):
        score = lax.dot_general(
            ent_ref[first : first + SUB, :],
            ql_ref[...],
            (((1,), (1,)), ((), ())),
            preferred_element_type=jnp.float32,
        )
        soft = 1.0 / (1.0 + jnp.exp(-sharpness * (score - row_ref[...])))
        acc_ref[...] += jnp.sum(soft.reshape(-1, 8, queries), axis=0)

    @pl.when(step == pl.num_programs(0) - 1)
    def _():
        o_ref[...] = old_ref[...]
        for k, block in enumerate(blocks):
            total = jnp.sum(acc_ref[:, k * piece : (k + 1) * piece], axis=0, keepdims=True)
            o_ref[pl.ds(block_class(block), 1), :] = total * weight


def soft_counts(blocks, weight, pieces, table, level, old):
    piece, width = pieces[0].shape
    queries = piece * len(pieces)
    rows = table.shape[0]
    eb = STEP // SPLIT
    whole = pl.BlockSpec(level.shape, lambda i: (0, 0))
    return pl.pallas_call(
        functools.partial(score_kernel, blocks, weight),
        grid=(rows // STEP,),
        in_specs=[pl.BlockSpec((piece, width), lambda i: (0, 0))] * len(pieces)
        + [pl.BlockSpec((eb, width), lambda i, j=j: (i * SPLIT + j, 0)) for j in range(SPLIT)]
        + [whole, whole],
        out_specs=whole,
        out_shape=jax.ShapeDtypeStruct(old.shape, jnp.float32),
        scratch_shapes=[
            pltpu.VMEM((queries, width), jnp.bfloat16),
            pltpu.VMEM((1, queries), jnp.float32),
            pltpu.VMEM((8, queries), jnp.float32),
            pltpu.VMEM((STEP, width), jnp.bfloat16),
        ],
        cost_estimate=pl.CostEstimate(
            flops=2 * queries * rows * width,
            transcendentals=2 * queries * rows,
            bytes_accessed=4 * width * (rows + queries),
        ),
        name="soft_counts",
    )(*pieces, *([table] * SPLIT), level, old)


def pick_rows(table, ids, start):
    count = table.shape[0]
    local = ids - start
    owned = (local >= 0) & (local < count)
    picked = jnp.take(table, jnp.clip(local, 0, count - 1), axis=0, mode="clip")
    return jnp.where(owned[:, None], picked, 0.0)


def shards(entity_table, relations, thresholds, head_ids, rel_ids, thr_idx):
    rows, width = entity_table.shape
    devices = lax.axis_size(ALL)
    queries = head_ids.shape[0]
    ents = rows * devices
    me = lax.axis_index(ALL)
    core = lax.axis_index("c")
    swap = [(0, 1), (1, 0)]
    start = me * rows
    home = queries // devices

    sizes = [lax.axis_size(a) for a in ALL]
    x = lax.axis_index("x")
    classes = lambda v: v.reshape(*sizes, home).transpose(0, 2, 1, 3, 4, 5).reshape(8, queries // 8)
    flat1 = flipped(entity_table, *PARTS[0])
    got1 = [flat1[0]] + [hopped(p, h) for p, h in zip(flat1[1:7], HOPS[1:7])]

    ids = classes(head_ids)
    owner = ids // rows
    local = ids - owner * rows
    members = queries // 8
    spot = jnp.arange(members)
    earlier = spot[None, None, :] < spot[None, :, None]

    def rank_of(key):
        same = key[:, :, None] == key[:, None, :]
        return jnp.sum((same & earlier).astype(jnp.int32), axis=2)

    rank = rank_of(owner)
    slot = jnp.arange(CAP)
    hit = (owner == me)[:, None, :] & (rank[:, None, :] == slot[None, :, None])
    wanted = jnp.sum(jnp.where(hit, local[:, None, :], 0), axis=2).reshape(-1)
    out_rows = jnp.take(entity_table, wanted, axis=0, mode="clip").reshape(8, CAP, width)
    found = exchange(out_rows, ("x", "c")).reshape(-1, width)
    got1 += [hopped(p, h) for p, h in zip(flat1[7:], HOPS[7:])]

    plane = (owner // 16) % 2 * 8 + owner % 8
    plane_rank = rank_of(plane)
    fits = (jnp.max(rank) < CAP) & (jnp.max(plane_rank) < CAP_YZ)
    source = owner // 32 * 2 + (owner // 8) % 2
    stack = jnp.stack([plane, plane_rank, source * CAP + rank, classes(rel_ids)])
    my_plane, my_rank, my_spot, my_rel = jnp.take(stack, x * 2 + core, axis=1)
    place = jnp.arange(CAP_YZ)[:, None]
    chosen = (my_plane == lax.axis_index(YZ))[None, :] & (my_rank[None, :] == place)
    from_spot = jnp.sum(jnp.where(chosen, my_spot[None, :], 0), axis=1)
    from_rel = jnp.sum(jnp.where(chosen, my_rel[None, :], 0), axis=1)
    back = my_plane * CAP_YZ + my_rank
    factor = jnp.take(relations, from_rel, axis=0, mode="clip")
    sent_rows = jnp.take(found, from_spot, axis=0, mode="clip") * factor

    def every_row(unused):
        full = pick_rows(entity_table, head_ids, start)
        full = exchange(full.reshape(devices, home, width), ALL)
        one_rel = lax.dynamic_slice(rel_ids, (me * home,), (home,))
        one = jnp.sum(full, axis=0) * jnp.take(relations, one_rel, axis=0, mode="clip")
        return spread(one, YZ).reshape(-1, width)

    flat2 = flipped(entity_table, *PARTS[1])
    query = spread(sent_rows, YZ).reshape(-1, width)
    query = jnp.take(query, back, axis=0, mode="clip")
    query = lax.cond(fits, lambda q: q, every_row, query)
    got2 = [flat2[0]] + [None] * 7
    for k in ORDER[:3]:
        got2[k] = hopped(flat2[k], HOPS[k])
    held = {(0, 0): query}
    for shift in SHIFTS[1:]:
        held[shift, 0] = lax.ppermute(query, "x", [(i, (i + shift) % 4) for i in range(4)])
    for k in ORDER[3:]:
        got2[k] = hopped(flat2[k], HOPS[k])
    for shift in SHIFTS:
        held[shift, 1] = lax.ppermute(held[shift, 0], "c", swap)

    hot = classes(thr_idx)[:, :, None] == jnp.arange(thresholds.shape[0])[None, None, :]
    level = jnp.sum(jnp.where(hot, thresholds[None, None, :], 0.0), axis=2)
    sums = jnp.zeros_like(level)
    for shifts in (SHIFTS[:1], SHIFTS[1:]):
        blocks = tuple((shift, side) for side in (0, 1) for shift in shifts)
        sums = soft_counts(blocks, 1.0 / ents, [held[b] for b in blocks], entity_table, level, sums)
    got = exchange(sums.reshape(devices, home), ("x", "c", "yl", "yh", "z"))
    fraction = jnp.sum(got, axis=0)

    first, second = PARTS[0][0], PARTS[1][0]
    spots = tuple((k, first) for k in range(8)) + ((0, second),)
    table = placed(got1 + got2[:1], spots, rows, None)
    table = placed(got2[1:], tuple((k, second) for k in range(1, 8)), rows, table)
    return (table.T, fraction)


def solution(mesh):
    fine = Mesh(mesh.devices.reshape(4, 2, 2, 2, 4), ALL)
    whole = P(ALL, None)

    return jax.shard_map(
        shards,
        mesh=fine,
        in_specs=(whole, P(), P(), P(), P(), P()),
        out_specs=(P(("x", "yl", "c"), DIM), P(ALL)),
        check_vma=False,
    )
```
